256 devices in a mesh: image: 4 (over y, x), row: 64 (over z, core).
Axes of the slice: x: 2, y: 2, z: 32, core: 2. Of those that a mesh axis runs over, the one named last changes fastest.
The devices are a block of a 4x8x32 slice.
Arguments:
- density: float32 [2048, 7, 128, 128], P(('image', 'row')), parts along dimension 0, as said below
- block_columns: int32 [2048, 7], P(('image', 'row')), parts along dimension 0, may hold values from -1 to 511, as said below
Outputs:
- purified: float32 [2048, 7, 128, 128], P(('image', 'row')), parts along dimension 0
- occupation: float32 [12], P('image'), parts along dimension 0
The draws below stay inside these ranges and needn't reach their ends.
There are 4 independent parts, one for each index of `image`. The reference program is written for one: setup_inputs(seed, part) draws one part's arguments, and reference() takes and returns one part's arrays. A program takes and returns all parts, laid end to end along the dimension named above; each array names one. Nothing has to cross between parts.
Inputs may be any that keep to these rules, and one draw needn't show every extreme that they name: `block_columns`: slot s of block row i holds block column i - 3 + s or is empty (-1); slot 3 (column i) is never empty, and no slot points outside the matrix; the pattern is symmetric (j is in row i exactly when i is in row j); every draw has rows with all 7 slots filled. The density matrix is symmetric: the block in slot s of row i is the transpose of the block of row j = block_columns[i, s] whose column is i, and every diagonal block is symmetric.
All inputs are finite; a program needn't handle non-finite values.
Results may differ from the reference program's by a relative error of at most 0.0003.
Values sent between devices are 32-bit elements; how exact they have to be, the bound alone decides.
No kernel may reach another device: no remote copies, remote signals or barrier semaphores. Data moves between devices by JAX's collectives and lax.ppermute only.
A program may use at most 128 MiB of HBM per device.

```python
import jax
import jax.numpy as jnp
from jax import lax

BS = 128
HALF = 3
STEPS = 2
K = 7
NB = 512
ORDER = 65536


def pattern(key):
    key_shift, key_roll = jax.random.split(key)
    shift = jax.random.randint(key_shift, (), 0, NB)
    row_ids = jnp.arange(NB, dtype=jnp.int32)
    chance = jnp.minimum(100, 25 + 100 * ((row_ids + shift) % NB) // NB)
    rolled = jax.random.randint(key_roll, (NB, HALF), 0, 100)
    offsets = jnp.arange(1, HALF + 1, dtype=jnp.int32)
    forward = (rolled < chance[:, None]) & (row_ids[:, None] + offsets[None, :] < NB)
    backward = []
    for offset in range(HALF, 0, -1):
        source = jnp.clip(row_ids - offset, 0, NB - 1)
        backward.append(jnp.where(row_ids - offset >= 0, forward[source, offset - 1], False))
    backward = jnp.stack(backward, 1)
    present = jnp.concatenate([backward, jnp.ones((NB, 1), dtype=bool), forward], 1)
    column_of = row_ids[:, None] + jnp.arange(-HALF, HALF + 1, dtype=jnp.int32)[None, :]
    return jnp.where(present, column_of, -1).astype(jnp.int32)


def symmetrize(jitter, columns):
    row_ids = jnp.arange(NB, dtype=jnp.int32)
    partners = []
    for slot in range(K):
        target = jnp.clip(row_ids - HALF + slot, 0, NB - 1).astype(jnp.int32)
        partners.append(jitter[target, K - 1 - slot])
    partner = jnp.stack(partners, 1)
    partner_t = jnp.swapaxes(partner, 2, 3)
    own_t = jnp.swapaxes(jitter, 2, 3)
    upper = (columns > row_ids[:, None]).astype(jnp.float32)[:, :, None, None]
    lower = ((columns < row_ids[:, None]) & (columns >= 0)).astype(jnp.float32)[:, :, None, None]
    diagonal = (columns == row_ids[:, None]).astype(jnp.float32)[:, :, None, None]
    return upper * jitter + lower * partner_t + diagonal * 0.5 * (jitter + own_t)


def draw_block_columns(key, part):
    return pattern(jax.random.fold_in(key, 7))


def draw_density(key, part):
    columns = pattern(jax.random.fold_in(key, 7))
    key_noise, key_diag = jax.random.split(jax.random.fold_in(key, 11))
    spread = 0.15 / (BS * K) ** 0.5
    jitter = jax.random.normal(key_noise, (NB, K, BS, BS), jnp.float32) * spread
    offset = jax.random.uniform(key_diag, (NB, BS), jnp.float32, -0.2, 0.2)
    jitter = symmetrize(jitter, columns)
    center = 0.25 + 0.5 * jnp.arange(NB, dtype=jnp.float32) / NB
    diagonal = center[:, None] + offset
    row_ids = jnp.arange(NB, dtype=jnp.int32)
    on_diagonal = (columns == row_ids[:, None]).astype(jnp.float32)
    identity = jnp.eye(BS, dtype=jnp.float32)
    blocks = jitter + on_diagonal[:, :, None, None] * (diagonal[:, None, :, None] * identity[None, None, :, :])
    return blocks * (columns >= 0).astype(jnp.float32)[:, :, None, None]


def setup_inputs(seed: int = 0, part: int = 0) -> dict:
    streams_of = jax.random.split(jax.random.key(seed), 3)
    own_keys = jax.random.split(jax.random.fold_in(streams_of[2], part), 3)
    density = draw_density(jax.random.fold_in(jax.random.fold_in(streams_of[2], part), 71), part)
    block_columns = draw_block_columns(jax.random.fold_in(jax.random.fold_in(streams_of[2], part), 71), part)
    return dict(density=density, block_columns=block_columns)


def pattern_product(first_rows, columns, second_rows):
    block_count = columns.shape[0]

    def one_row(packed):
        row_blocks, row_columns = packed
        present = row_columns >= 0
        where_rows = jnp.clip(row_columns, 0, block_count - 1).astype(jnp.int32)
        picked = second_rows[where_rows]
        picked_columns = columns[where_rows]
        matches = (picked_columns[None, :, :] == row_columns[:, None, None]) & present[:, None, None] & present[None, :, None]
        products = jnp.einsum('bxy,bsyz->bsxz', row_blocks, picked, precision=lax.Precision.HIGHEST)
        return jnp.einsum('abs,bsxz->axz', matches.astype(jnp.float32), products, precision=lax.Precision.HIGHEST)

    return lax.map(one_row, (first_rows, columns))


def full_trace(blocks, columns):
    row_ids = jnp.arange(columns.shape[0], dtype=jnp.int32)
    on_diagonal = (columns == row_ids[:, None]).astype(jnp.float32)
    return jnp.sum(on_diagonal * jnp.trace(blocks, axis1=2, axis2=3))


def reference(density, block_columns):
    present = (block_columns >= 0).astype(jnp.float32)
    current = density * present[:, :, None, None]
    traces = [full_trace(current, block_columns) / ORDER]
    for number in range(STEPS):
        square = pattern_product(current, block_columns, current)
        cube_term = pattern_product(square, block_columns, current)
        current = 3.0 * square - 2.0 * cube_term
        traces.append(full_trace(current, block_columns) / ORDER)
    return current, jnp.stack(traces)
```

```python
import functools

import jax
import jax.numpy as jnp
from jax import lax
from jax.experimental import pallas as pl
from jax.experimental.pallas import tpu as pltpu
from jax.sharding import PartitionSpec as P

HALF = 3
STEPS = 2
PAD = 4
TRIANGLE = [(a, b) for a in range(HALF) for b in range(a, HALF)]


def low_edge():
    return [(a, s) for a in range(HALF) for s in range(0, 2 * HALF - a)]


def high_edge(rows):
    return [(rows - HALF + a, s) for a in range(HALF) for s in range(HALF - a, 2 * HALF + 1)]


def split(value):
    high = value.astype(jnp.bfloat16)
    return high, (value - high.astype(jnp.float32)).astype(jnp.bfloat16)


def edge_kernel(columns_ref, *refs):
    blocks, outs = refs[: 4 * HALF], refs[4 * HALF :]
    rows = columns_ref.shape[0]
    for side, (out, base) in enumerate(zip(outs, (0, rows - HALF))):
        for n, (a, b) in enumerate(TRIANGLE):
            keep = (columns_ref[base + a, HALF + b - a] >= 0).astype(jnp.float32)
            out[n] = blocks[side * len(TRIANGLE) + n][0, 0] * keep


def edges(density, columns):
    rows, _, size, _ = density.shape
    picks = [(base + a, HALF + b - a) for base in (0, rows - HALF) for a, b in TRIANGLE]
    shape = jax.ShapeDtypeStruct((len(TRIANGLE), size, size), jnp.float32)
    specs = [pl.BlockSpec((1, 1, size, size), lambda g, r=r, s=s: (r, s, 0, 0)) for r, s in picks]
    whole = pl.BlockSpec((len(TRIANGLE), size, size), lambda g: (0, 0, 0))
    return pl.pallas_call(
        edge_kernel,
        grid=(1,),
        in_specs=[pl.BlockSpec(memory_space=pltpu.SMEM)] + specs,
        out_specs=[whole, whole],
        out_shape=[shape, shape],
        name="edges",
    )(columns, *([density] * len(picks)))


def diagonal_lanes(block):
    size = block.shape[0]
    eye = lax.broadcasted_iota(jnp.int32, (size, size), 0) == lax.broadcasted_iota(jnp.int32, (size, size), 1)
    return jnp.sum(jnp.where(eye, block, 0.0), axis=0, keepdims=True)


def step_kernel(first, columns_ref, p_ref, before_ref, after_ref, out_ref, *rest):
    rows, slots, size, _ = p_ref.shape
    window = rows + 2 * PAD
    if first:
        low_ref, high_ref, trace_ref, dh, dl, sh, sl = rest
    else:
        trace_ref, dh, dl, sh, sl = rest

    def keep(i, s):
        return (columns_ref[i, s] >= 0).astype(jnp.float32)

    def area(ref, p, q):
        return ref.at[p * size : (p + 1) * size, q * size : (q + 1) * size]

    def put(p, q, value):
        high, low = split(value)
        area(dh, p, q)[...] = high
        area(dl, p, q)[...] = low

    filled = set()
    old_trace = jnp.zeros((1, size), jnp.float32)
    for i in range(rows):
        for s in range(slots):
            block = p_ref[i, s]
            if first:
                block = block * keep(i, s)
            if s == HALF:
                old_trace += diagonal_lanes(block)
            p, q = PAD + i, PAD + i + s - HALF
            put(p, q, block)
            filled.add((p, q))
            if first and not PAD <= q < PAD + rows:
                put(q, p, block.T)
                filled.add((q, p))
    if first:
        for ref, base in ((before_ref, PAD - HALF), (after_ref, PAD + rows)):
            for n, (a, b) in enumerate(TRIANGLE):
                block = ref[n]
                put(base + a, base + b, block)
                filled.add((base + a, base + b))
                if a != b:
                    put(base + b, base + a, block.T)
                    filled.add((base + b, base + a))
    else:
        for ref, picks, shift in (
            (before_ref, high_edge(rows), PAD - rows),
            (after_ref, low_edge(), PAD + rows),
        ):
            for n, (i, s) in enumerate(picks):
                p = i + shift
                put(p, p + s - HALF, ref[n])
                filled.add((p, p + s - HALF))
    zero = jnp.zeros((size, size), jnp.bfloat16)
    for p in range(window):
        for q in range(window):
            if abs(p // 2 - q // 2) <= 2 and (p, q) not in filled:
                area(dh, p, q)[...] = zero
                area(dl, p, q)[...] = zero
    for i in range(rows):
        for q in range(window):
            if abs((PAD + i) // 2 - q // 2) <= 2 and abs(PAD + i - q) > HALF:
                area(sh, i, q)[...] = zero
                area(sl, i, q)[...] = zero

    def product(xh, xl, shift, write):
        for i in range(rows):
            p = PAD + i
            first_pair, last_pair = (p - HALF) // 2, (p + HALF) // 2
            for pair in range(first_pair, last_pair + 1):
                j0, j1 = max(first_pair, pair - 2), min(last_pair, pair + 2)
                if 2 * pair + 1 < p - HALF + 1:
                    j1 = min(j1, (2 * pair + 1 + HALF) // 2)
                if 2 * pair > p + HALF - 1:
                    j0 = max(j0, (2 * pair - HALF) // 2)
                inner = slice(2 * j0 * size, 2 * (j1 + 1) * size)
                across = slice(2 * pair * size, 2 * (pair + 1) * size)
                mine = slice((i + shift) * size, (i + shift + 1) * size)
                ah, al = xh[mine, inner], xl[mine, inner]
                bh, bl = dh[inner, across], dl[inner, across]
                dot = functools.partial(jnp.dot, preferred_element_type=jnp.float32)
                total = dot(ah, bh) + dot(ah, bl) + dot(al, bh)
                for half in range(2):
                    s = 2 * pair + half - p + HALF
                    if 0 <= s < slots:
                        write(i, s, total[:, half * size : (half + 1) * size] * keep(i, s))

    def write_square(i, s, block):
        out_ref[i, s] = block
        high, low = split(block)
        area(sh, i, PAD + i + s - HALF)[...] = high
        area(sl, i, PAD + i + s - HALF)[...] = low

    product(dh, dl, PAD, write_square)
    traces = []

    def write_next(i, s, cube):
        block = 3.0 * out_ref[i, s] - 2.0 * cube
        out_ref[i, s] = block
        if s == HALF:
            traces.append(diagonal_lanes(block))
        if first:
            for ref, picks in ((low_ref, low_edge()), (high_ref, high_edge(rows))):
                if (i, s) in picks:
                    ref[picks.index((i, s))] = block

    product(sh, sl, 0, write_next)
    new_trace = sum(traces[1:], traces[0])
    trace_ref[...] = jnp.zeros(trace_ref.shape, jnp.float32)
    if first:
        trace_ref[0:1, :] = old_trace
        trace_ref[1:2, :] = new_trace
    else:
        trace_ref[2:3, :] = new_trace


def step(first, columns, current, before, after):
    rows, slots, size, _ = current.shape
    window = rows + 2 * PAD
    f32 = jnp.float32
    outs = [jax.ShapeDtypeStruct(current.shape, f32)]
    if first:
        outs += [jax.ShapeDtypeStruct((len(low_edge()), size, size), f32)] * 2
    outs += [jax.ShapeDtypeStruct((8, size), f32)]
    vmem = pl.BlockSpec(memory_space=pltpu.VMEM)
    return pl.pallas_call(
        functools.partial(step_kernel, first),
        in_specs=[pl.BlockSpec(memory_space=pltpu.SMEM), vmem, vmem, vmem],
        out_specs=[vmem] * len(outs),
        out_shape=outs,
        scratch_shapes=[pltpu.VMEM((window * size, window * size), jnp.bfloat16)] * 2
        + [pltpu.VMEM((rows * size, window * size), jnp.bfloat16)] * 2,
        compiler_params=pltpu.CompilerParams(vmem_limit_bytes=60 * 1024 * 1024),
        name="first_step" if first else "second_step",
    )(columns, current, before, after)


def over_rows(x):
    count = lax.axis_size("row")
    stride = 1
    for length in (2, 4, count // 8):
        groups = [
            [base + k * stride for k in range(length)]
            for base in range(count)
            if (base // stride) % length == 0
        ]
        x = lax.psum(x, "row", axis_index_groups=groups)
        stride *= length
    return x


def on_device(density, block_columns):
    order_total = lax.axis_size("row") * density.shape[0] * density.shape[2]
    count = lax.axis_size("row")
    up = [(i, i + 1) for i in range(count - 1)]
    down = [(j, i) for i, j in up]
    low, high = edges(density, block_columns)
    before, after = lax.ppermute(high, "row", up), lax.ppermute(low, "row", down)
    current, low, high, early = step(True, block_columns, density, before, after)
    before, after = lax.ppermute(high, "row", up), lax.ppermute(low, "row", down)
    current, late = step(False, block_columns, current, before, after)
    traces = jnp.sum(over_rows(early + late), axis=1)[: STEPS + 1]
    return current, traces / order_total


def solution(mesh):
    in_specs = (P(("image", "row"), None, None, None), P(("image", "row"), None))
    out_specs = (P(("image", "row"), None, None, None), P("image"))
    return jax.shard_map(
        on_device, mesh=mesh, in_specs=in_specs, out_specs=out_specs, check_vma=False
    )
```

```python
import functools

import jax
import jax.numpy as jnp
from jax import lax
from jax.experimental import pallas as pl
from jax.experimental.pallas import tpu as pltpu
from jax.sharding import PartitionSpec as P

HALF = 3
STEPS = 2
PAD = 4
TRIANGLE = [(a, b) for a in range(HALF) for b in range(a, HALF)]


def low_edge():
    return [(a, s) for a in range(HALF) for s in range(0, 2 * HALF - a)]


def high_edge(rows):
    return [(rows - HALF + a, s) for a in range(HALF) for s in range(HALF - a, 2 * HALF + 1)]


def split(value):
    high = value.astype(jnp.bfloat16)
    return high, (value - high.astype(jnp.float32)).astype(jnp.bfloat16)


def edge_kernel(columns_ref, *refs):
    blocks, outs = refs[: 4 * HALF], refs[4 * HALF :]
    rows = columns_ref.shape[0]
    for side, (out, base) in enumerate(zip(outs, (0, rows - HALF))):
        for n, (a, b) in enumerate(TRIANGLE):
            keep = (columns_ref[base + a, HALF + b - a] >= 0).astype(jnp.float32)
            out[n] = blocks[side * len(TRIANGLE) + n][0, 0] * keep


def edges(density, columns):
    rows, _, size, _ = density.shape
    picks = [(base + a, HALF + b - a) for base in (0, rows - HALF) for a, b in TRIANGLE]
    shape = jax.ShapeDtypeStruct((len(TRIANGLE), size, size), jnp.float32)
    specs = [pl.BlockSpec((1, 1, size, size), lambda g, r=r, s=s: (r, s, 0, 0)) for r, s in picks]
    whole = pl.BlockSpec((len(TRIANGLE), size, size), lambda g: (0, 0, 0))
    return pl.pallas_call(
        edge_kernel,
        grid=(1,),
        in_specs=[pl.BlockSpec(memory_space=pltpu.SMEM)] + specs,
        out_specs=[whole, whole],
        out_shape=[shape, shape],
        name="edges",
    )(columns, *([density] * len(picks)))


def diagonal_lanes(block):
    size = block.shape[0]
    eye = lax.broadcasted_iota(jnp.int32, (size, size), 0) == lax.broadcasted_iota(jnp.int32, (size, size), 1)
    return jnp.sum(jnp.where(eye, block, 0.0), axis=0, keepdims=True)


def step_kernel(first, columns_ref, p_ref, before_ref, after_ref, *rest):
    if first:
        out_ref, low_ref, high_ref, trace_ref, dh, dl, sh, sl = rest
    else:
        early_ref, out_hbm, trace_ref, out_ref, dh, dl, sh, sl, out_sems = rest
    rows, slots, size, _ = p_ref.shape
    window = rows + 2 * PAD

    def keep(i, s):
        return (columns_ref[i, s] >= 0).astype(jnp.float32)

    def area(ref, p, q):
        return ref.at[p * size : (p + 1) * size, q * size : (q + 1) * size]

    def put(p, q, value):
        high, low = split(value)
        area(dh, p, q)[...] = high
        area(dl, p, q)[...] = low

    zero = jnp.zeros((size, size), jnp.bfloat16)
    last = PAD + rows + HALF
    for p in range(window):
        for q in range(window):
            inside = PAD - HALF <= min(p, q) and max(p, q) < last and abs(p - q) <= HALF
            if abs(p // 2 - q // 2) <= 2 and not inside:
                area(dh, p, q)[...] = zero
                area(dl, p, q)[...] = zero
    for i in range(rows):
        for q in range(window):
            if abs((PAD + i) // 2 - q // 2) <= 2 and abs(PAD + i - q) > HALF:
                area(sh, i, q)[...] = zero
                area(sl, i, q)[...] = zero

    old_trace = jnp.zeros((1, size), jnp.float32)
    for i in range(rows):
        for s in range(slots):
            block = p_ref[i, s]
            if first:
                block = block * keep(i, s)
                if s == HALF:
                    old_trace += diagonal_lanes(block)
            p, q = PAD + i, PAD + i + s - HALF
            put(p, q, block)
            if first and not PAD <= q < PAD + rows:
                put(q, p, block.T)
    if first:
        for ref, base in ((before_ref, PAD - HALF), (after_ref, PAD + rows)):
            for n, (a, b) in enumerate(TRIANGLE):
                block = ref[n]
                put(base + a, base + b, block)
                if a != b:
                    put(base + b, base + a, block.T)
    else:
        for ref, picks, shift in (
            (before_ref, high_edge(rows), PAD - rows),
            (after_ref, low_edge(), PAD + rows),
        ):
            for n, (i, s) in enumerate(picks):
                p = i + shift
                put(p, p + s - HALF, ref[n])

    def product(xh, xl, shift, write, leave):
        for i in range(rows):
            p = PAD + i
            first_pair, last_pair = (p - HALF) // 2, (p + HALF) // 2
            for pair in range(first_pair, last_pair + 1):
                j0, j1 = max(first_pair, pair - 2), min(last_pair, pair + 2)
                if 2 * pair + 1 < p - HALF + 1:
                    j1 = min(j1, (2 * pair + 1 + HALF) // 2)
                if 2 * pair > p + HALF - 1:
                    j0 = max(j0, (2 * pair - HALF) // 2)
                inner = slice(2 * j0 * size, 2 * (j1 + 1) * size)
                across = slice(2 * pair * size, 2 * (pair + 1) * size)
                mine = slice((i + shift) * size, (i + shift + 1) * size)
                ah, al = xh[mine, inner], xl[mine, inner]
                bh, bl = dh[inner, across], dl[inner, across]
                dot = functools.partial(jnp.dot, preferred_element_type=jnp.float32)
                total = dot(ah, bh) + dot(ah, bl) + dot(al, bh)
                for half in range(2):
                    s = 2 * pair + half - p + HALF
                    if 0 <= s < slots:
                        write(i, s, total[:, half * size : (half + 1) * size] * keep(i, s))
            if i:
                leave(i - 1)

    def write_square(i, s, block):
        out_ref[i, s] = block
        high, low = split(block)
        area(sh, i, PAD + i + s - HALF)[...] = high
        area(sl, i, PAD + i + s - HALF)[...] = low

    product(dh, dl, PAD, write_square, lambda i: None)
    traces = []

    def write_next(i, s, cube):
        block = 3.0 * out_ref[i, s] - 2.0 * cube
        out_ref[i, s] = block
        if s == HALF:
            traces.append(diagonal_lanes(block))

    leaving = []

    def leave(i):
        if first:
            for edge_ref, picks in ((low_ref, low_edge()), (high_ref, high_edge(rows))):
                for n, (row, s) in enumerate(picks):
                    if row == i:
                        edge_ref[n] = out_ref[i, s]
            return
        copy = pltpu.make_async_copy(out_ref.at[i], out_hbm.at[i], out_sems.at[i])
        copy.start()
        leaving.append(copy)

    product(sh, sl, 0, write_next, leave)
    new_trace = sum(traces[1:], traces[0])
    if first:
        trace_ref[...] = jnp.zeros(trace_ref.shape, jnp.float32)
        trace_ref[0:1, :] = old_trace
        trace_ref[1:2, :] = new_trace
    else:
        trace_ref[...] = early_ref[...]
        trace_ref[2:3, :] = new_trace
    leave(rows - 1)
    for copy in leaving:
        copy.wait()


def step(first, columns, current, before, after, early=None):
    rows, slots, size, _ = current.shape
    window = rows + 2 * PAD
    f32 = jnp.float32
    vmem = pl.BlockSpec(memory_space=pltpu.VMEM)
    dense = [pltpu.VMEM((window * size, window * size), jnp.bfloat16)] * 2
    dense += [pltpu.VMEM((rows * size, window * size), jnp.bfloat16)] * 2
    traces = jax.ShapeDtypeStruct((8, size), f32)
    if first:
        edge = jax.ShapeDtypeStruct((len(low_edge()), size, size), f32)
        outs, out_specs = [jax.ShapeDtypeStruct(current.shape, f32), edge, edge, traces], [vmem] * 4
        scratch = dense
    else:
        outs = [jax.ShapeDtypeStruct(current.shape, f32), traces]
        out_specs = [pl.BlockSpec(memory_space=pl.ANY), vmem]
        scratch = [pltpu.VMEM(current.shape, f32)] + dense + [pltpu.SemaphoreType.DMA((rows,))]
    return pl.pallas_call(
        functools.partial(step_kernel, first),
        in_specs=[pl.BlockSpec(memory_space=pltpu.SMEM)] + [vmem] * (3 if first else 4),
        out_specs=out_specs,
        out_shape=outs,
        scratch_shapes=scratch,
        compiler_params=pltpu.CompilerParams(vmem_limit_bytes=44 * 1024 * 1024),
        name="first_step" if first else "second_step",
    )(columns, current, before, after, *([] if first else [early]))


def over_rows(x):
    count = lax.axis_size("row")
    stride = 1
    for length in (2, 4, count // 8):
        groups = [
            [base + k * stride for k in range(length)]
            for base in range(count)
            if (base // stride) % length == 0
        ]
        x = lax.psum(x, "row", axis_index_groups=groups)
        stride *= length
    return x


def on_device(density, block_columns):
    order_total = lax.axis_size("row") * density.shape[0] * density.shape[2]
    count = lax.axis_size("row")
    up = [(i, i + 1) for i in range(count - 1)]
    down = [(j, i) for i, j in up]
    low, high = edges(density, block_columns)
    before, after = lax.ppermute(high, "row", up), lax.ppermute(low, "row", down)
    current, low, high, early = step(True, block_columns, density, before, after)
    before, after = lax.ppermute(high, "row", up), lax.ppermute(low, "row", down)
    current, traces = step(False, block_columns, current, before, after, early)
    traces = jnp.sum(over_rows(traces), axis=1)[: STEPS + 1]
    return current, traces / order_total


def solution(mesh):
    in_specs = (P(("image", "row"), None, None, None), P(("image", "row"), None))
    out_specs = (P(("image", "row"), None, None, None), P("image"))
    return jax.shard_map(
        on_device, mesh=mesh, in_specs=in_specs, out_specs=out_specs, check_vma=False
    )
```

```python
import functools

import jax
import jax.numpy as jnp
from jax import lax
from jax.experimental import pallas as pl
from jax.experimental.pallas import tpu as pltpu
from jax.sharding import PartitionSpec as P

HALF = 3
STEPS = 2
PAD = 4
TRIANGLE = [(a, b) for a in range(HALF) for b in range(a, HALF)]


def low_edge():
    return [(a, s) for a in range(HALF) for s in range(0, 2 * HALF - a)]


def high_edge(rows):
    return [(rows - HALF + a, s) for a in range(HALF) for s in range(HALF - a, 2 * HALF + 1)]


def split(value):
    high = value.astype(jnp.bfloat16)
    return high, (value - high.astype(jnp.float32)).astype(jnp.bfloat16)


def edge_kernel(columns_ref, *refs):
    blocks, outs = refs[: 4 * HALF], refs[4 * HALF :]
    rows = columns_ref.shape[0]
    for side, (out, base) in enumerate(zip(outs, (0, rows - HALF))):
        for n, (a, b) in enumerate(TRIANGLE):
            keep = (columns_ref[base + a, HALF + b - a] >= 0).astype(jnp.float32)
            out[n] = blocks[side * len(TRIANGLE) + n][0, 0] * keep


def edges(density, columns):
    rows, _, size, _ = density.shape
    picks = [(base + a, HALF + b - a) for base in (0, rows - HALF) for a, b in TRIANGLE]
    shape = jax.ShapeDtypeStruct((len(TRIANGLE), size, size), jnp.float32)
    specs = [pl.BlockSpec((1, 1, size, size), lambda g, r=r, s=s: (r, s, 0, 0)) for r, s in picks]
    whole = pl.BlockSpec((len(TRIANGLE), size, size), lambda g: (0, 0, 0))
    return pl.pallas_call(
        edge_kernel,
        grid=(1,),
        in_specs=[pl.BlockSpec(memory_space=pltpu.SMEM)] + specs,
        out_specs=[whole, whole],
        out_shape=[shape, shape],
        name="edges",
    )(columns, *([density] * len(picks)))


def diagonal_lanes(block):
    size = block.shape[0]
    eye = lax.broadcasted_iota(jnp.int32, (size, size), 0) == lax.broadcasted_iota(jnp.int32, (size, size), 1)
    return jnp.sum(jnp.where(eye, block, 0.0), axis=0, keepdims=True)


def step_kernel(first, columns_ref, p_ref, before_ref, after_ref, *rest):
    if first:
        out_ref, low_ref, high_ref, trace_ref, dh, dl, sh, sl = rest
    else:
        early_ref, out_hbm, trace_ref, out_ref, dh, dl, sh, sl, out_sems = rest
    rows, slots, size, _ = p_ref.shape
    window = rows + 2 * PAD

    def keep(i, s):
        return (columns_ref[i, s] >= 0).astype(jnp.float32)

    def area(ref, p, q):
        return ref.at[p * size : (p + 1) * size, q * size : (q + 1) * size]

    def put(p, q, value):
        high, low = split(value)
        area(dh, p, q)[...] = high
        area(dl, p, q)[...] = low

    zero = jnp.zeros((size, size), jnp.bfloat16)
    last = PAD + rows + HALF
    for p in range(window):
        for q in range(window):
            inside = PAD - HALF <= min(p, q) and max(p, q) < last and abs(p - q) <= HALF
            if abs(p // 2 - q // 2) <= 2 and not inside:
                area(dh, p, q)[...] = zero
                area(dl, p, q)[...] = zero
    for i in range(rows):
        for q in range(window):
            if abs((PAD + i) // 2 - q // 2) <= 2 and abs(PAD + i - q) > HALF:
                area(sh, i, q)[...] = zero
                area(sl, i, q)[...] = zero

    old_trace = jnp.zeros((1, size), jnp.float32)
    for i in range(rows):
        for s in range(slots):
            block = p_ref[i, s]
            if first:
                block = block * keep(i, s)
                if s == HALF:
                    old_trace += diagonal_lanes(block)
            p, q = PAD + i, PAD + i + s - HALF
            put(p, q, block)
            if first and not PAD <= q < PAD + rows:
                put(q, p, block.T)
    if first:
        for ref, base in ((before_ref, PAD - HALF), (after_ref, PAD + rows)):
            for n, (a, b) in enumerate(TRIANGLE):
                block = ref[n]
                put(base + a, base + b, block)
                if a != b:
                    put(base + b, base + a, block.T)
    else:
        for ref, picks, shift in (
            (before_ref, high_edge(rows), PAD - rows),
            (after_ref, low_edge(), PAD + rows),
        ):
            for n, (i, s) in enumerate(picks):
                p = i + shift
                put(p, p + s - HALF, ref[n])

    def product(xh, xl, shift, write, leave):
        for i in range(rows):
            p = PAD + i
            first_pair, last_pair = (p - HALF) // 2, (p + HALF) // 2
            for pair in range(first_pair, last_pair + 1):
                j0, j1 = max(first_pair, pair - 2), min(last_pair, pair + 2)
                if 2 * pair + 1 < p - HALF + 1:
                    j1 = min(j1, (2 * pair + 1 + HALF) // 2)
                if 2 * pair > p + HALF - 1:
                    j0 = max(j0, (2 * pair - HALF) // 2)
                inner = slice(2 * j0 * size, 2 * (j1 + 1) * size)
                across = slice(2 * pair * size, 2 * (pair + 1) * size)
                mine = slice((i + shift) * size, (i + shift + 1) * size)
                ah, al = xh[mine, inner], xl[mine, inner]
                bh, bl = dh[inner, across], dl[inner, across]
                dot = functools.partial(jnp.dot, preferred_element_type=jnp.float32)
                total = dot(ah, bh) + dot(ah, bl) + dot(al, bh)
                for half in range(2):
                    s = 2 * pair + half - p + HALF
                    if 0 <= s < slots:
                        write(i, s, total[:, half * size : (half + 1) * size] * keep(i, s))
            if i:
                leave(i - 1)

    def write_square(i, s, block):
        out_ref[i, s] = block
        high, low = split(block)
        area(sh, i, PAD + i + s - HALF)[...] = high
        area(sl, i, PAD + i + s - HALF)[...] = low

    product(dh, dl, PAD, write_square, lambda i: None)
    traces = []

    def write_next(i, s, cube):
        block = 3.0 * out_ref[i, s] - 2.0 * cube
        out_ref[i, s] = block
        if s == HALF:
            traces.append(diagonal_lanes(block))

    leaving = []

    def leave(i):
        if first:
            for edge_ref, picks in ((low_ref, low_edge()), (high_ref, high_edge(rows))):
                for n, (row, s) in enumerate(picks):
                    if row == i:
                        edge_ref[n] = out_ref[i, s]
            return
        copy = pltpu.make_async_copy(out_ref.at[i], out_hbm.at[i], out_sems.at[i])
        copy.start()
        leaving.append(copy)

    product(sh, sl, 0, write_next, leave)
    new_trace = sum(traces[1:], traces[0])
    if first:
        trace_ref[...] = jnp.zeros(trace_ref.shape, jnp.float32)
        trace_ref[0:1, :] = old_trace
        trace_ref[1:2, :] = new_trace
    else:
        trace_ref[...] = early_ref[...]
        trace_ref[2:3, :] = new_trace
    leave(rows - 1)
    for copy in leaving:
        copy.wait()


def step(first, columns, current, before, after, early=None):
    rows, slots, size, _ = current.shape
    window = rows + 2 * PAD
    f32 = jnp.float32
    vmem = pl.BlockSpec(memory_space=pltpu.VMEM)
    dense = [pltpu.VMEM((window * size, window * size), jnp.bfloat16)] * 2
    dense += [pltpu.VMEM((rows * size, window * size), jnp.bfloat16)] * 2
    traces = jax.ShapeDtypeStruct((8, size), f32)
    if first:
        edge = jax.ShapeDtypeStruct((len(low_edge()), size, size), f32)
        outs, out_specs = [jax.ShapeDtypeStruct(current.shape, f32), edge, edge, traces], [vmem] * 4
        scratch = dense
    else:
        outs = [jax.ShapeDtypeStruct(current.shape, f32), traces]
        out_specs = [pl.BlockSpec(memory_space=pl.ANY), vmem]
        scratch = [pltpu.VMEM(current.shape, f32)] + dense + [pltpu.SemaphoreType.DMA((rows,))]
    return pl.pallas_call(
        functools.partial(step_kernel, first),
        in_specs=[pl.BlockSpec(memory_space=pltpu.SMEM)] + [vmem] * (3 if first else 4),
        out_specs=out_specs,
        out_shape=outs,
        scratch_shapes=scratch,
        compiler_params=pltpu.CompilerParams(vmem_limit_bytes=44 * 1024 * 1024),
        name="first_step" if first else "second_step",
    )(columns, current, before, after, *([] if first else [early]))


def over_rows(x):
    count = lax.axis_size("row")
    for length, stride in ((count // 8, 8), (4, 2), (2, 1)):
        groups = [
            [base + k * stride for k in range(length)]
            for base in range(count)
            if (base // stride) % length == 0
        ]
        x = lax.psum(x, "row", axis_index_groups=groups)
    return x


def on_device(density, block_columns):
    order_total = lax.axis_size("row") * density.shape[0] * density.shape[2]
    count = lax.axis_size("row")
    up = [(i, i + 1) for i in range(count - 1)]
    down = [(j, i) for i, j in up]
    low, high = edges(density, block_columns)
    before, after = lax.ppermute(high, "row", up), lax.ppermute(low, "row", down)
    current, low, high, early = step(True, block_columns, density, before, after)
    before, after = lax.ppermute(high, "row", up), lax.ppermute(low, "row", down)
    current, traces = step(False, block_columns, current, before, after, early)
    traces = jnp.sum(over_rows(traces), axis=1)[: STEPS + 1]
    return current, traces / order_total


def solution(mesh):
    in_specs = (P(("image", "row"), None, None, None), P(("image", "row"), None))
    out_specs = (P(("image", "row"), None, None, None), P("image"))
    return jax.shard_map(
        on_device, mesh=mesh, in_specs=in_specs, out_specs=out_specs, check_vma=False
    )
```
